32 devices in a mesh: ccd: 16 (over z, y, x), row: 2 (over core).
Axes of the slice: x: 2, y: 2, z: 4, core: 2. Of those that a mesh axis runs over, the one named last changes fastest.
Arguments:
- exposure: float32 [16, 48, 2048], P('ccd', 'row'), may hold values from -6 to 6
- row_shift: int32 [16], P('ccd'), may hold values from 0 to 7
- row_fraction: bfloat16 [16, 48], P('ccd', 'row'), may hold values from 0 to 1
- column_shift: int32 [16], P('ccd'), may hold values from 0 to 127
- column_fraction: bfloat16 [16, 2048], P('ccd'), may hold values from 0 to 1
- piece_width: int32 [16, 16], P('ccd'), may hold values from 1 to 128
- route_tile: int32 [16, 16], P('ccd'), may hold values from 0 to 15, as said below
- route_cell: int32 [16, 16], P('ccd'), may hold values from 0 to 31, as said below
- template: float32 [16, 48, 4096], P('ccd', 'row'), may hold values from -6 to 6
- match_kernel: bfloat16 [16, 41, 41], P('ccd'), may hold values from -0.15625 to 0.15625
- detection_kernel: bfloat16 [16, 15, 15], P('ccd'), may hold values from -0.375 to 0.375
Outputs:
- difference: float32 [16, 48, 4096], P('ccd', 'row')
- significance: float32 [16, 48, 4096], P('ccd', 'row')
- noise_level: float32 [], replicated
The draws below stay inside these ranges and needn't reach their ends.
Inputs may be any that keep to these rules, and one draw needn't show every extreme that they name: Piece p of CCD c lands on tile route_tile[c, p]. Every tile receives at least one piece and at most 32 pieces in all; a quarter of the tiles receive exactly 32. No CCD puts more than 2 pieces on one tile, and some CCDs put exactly 2. `route_cell`: pieces that land on one tile fill different cells.
All inputs are finite; a program needn't handle non-finite values.
Results may differ from the reference program's by a relative error of at most 0.0044.
Values may be sent and summed in bfloat16 or wider, within the bound.
A program may use at most 128 MiB of HBM per device.

```python
import jax
import jax.numpy as jnp
from jax import lax

W = 2048
PW = 128
NP = 16
CROWS = 48
CCDS = 16
NT = 16
CAP = 32
HALO = 8
KS = 41
DK = 15


def route_tables(key):
    key_order = jax.random.fold_in(key, 101)
    key_pattern = jax.random.fold_in(key, 102)
    key_piece = jax.random.fold_in(key, 103)
    key_cell = jax.random.fold_in(key, 104)
    groups = CCDS // 4
    spreads = jax.random.randint(key_pattern, (groups,), 0, NP // 2).astype(jnp.int32)
    loads = jnp.stack([jnp.full((groups,), 2 * NP, jnp.int32), NP - spreads, NP // 2 + spreads, jnp.full((groups,), NP - NP // 2, jnp.int32)], axis=1).reshape(-1).astype(jnp.int32)
    order = jax.random.permutation(key_order, CCDS).astype(jnp.int32)
    ends = jnp.cumsum(loads).astype(jnp.int32)
    token = jnp.arange(CCDS * NP, dtype=jnp.int32)
    position = jnp.searchsorted(ends, token, side='right').astype(jnp.int32)
    piece_rank = token - (ends[position] - loads[position])
    tile_flat = order[position]
    spots = jax.random.randint(key_cell, (CCDS, CAP), 0, 1 << 20).astype(jnp.int32) * CAP + jnp.arange(CAP, dtype=jnp.int32)[None, :]
    cell_order = jnp.argsort(spots, axis=1).astype(jnp.int32)
    cell_flat = cell_order.reshape(-1)[tile_flat * CAP + piece_rank]
    tile_grid = tile_flat.reshape(NP // 2, CCDS, 2).transpose(1, 0, 2).reshape(CCDS, NP)
    cell_grid = cell_flat.reshape(NP // 2, CCDS, 2).transpose(1, 0, 2).reshape(CCDS, NP)
    scores = jax.random.randint(key_piece, (CCDS, NP), 0, 1 << 20).astype(jnp.int32) * NP + jnp.arange(NP, dtype=jnp.int32)[None, :]
    shuffle = jnp.argsort(scores, axis=1).astype(jnp.int32)
    return (jnp.take_along_axis(tile_grid, shuffle, axis=1).astype(jnp.int32), jnp.take_along_axis(cell_grid, shuffle, axis=1).astype(jnp.int32))


def draw_route_tile(key, part):
    return route_tables(key)[0]


def draw_route_cell(key, part):
    return route_tables(key)[1]


def place_ends(array, rng, smallest, largest):
    longest = array.shape.index(max(array.shape))
    spots = []
    for shift in (0, 1):
        where = [jax.random.randint(jax.random.fold_in(rng, axis), (), 0, length) for axis, length in enumerate(array.shape)]
        where[longest] = (where[longest] + shift) % array.shape[longest]
        spots.append(tuple(where))
    return array.at[spots[0]].set(smallest).at[spots[1]].set(largest)


def block_levels(key, extent, shards, least, high):
    loudness = 1.0
    for axis_at, shards_of in shards:
        steps = jax.random.uniform(jax.random.fold_in(jax.random.fold_in(key, 6), axis_at), (shards_of,), jnp.float32, least / len(shards), high / len(shards))
        loudness = loudness * jnp.repeat(jnp.exp(steps), extent[axis_at] // shards_of).reshape((-1,) + (1,) * (len(extent) - 1 - axis_at))
    return loudness


def gaussian(own_key, shape, scale, most, cuts=(), kind=jnp.bfloat16):
    array = scale * jax.random.normal(own_key, shape, jnp.float32)
    if cuts:
        array = array * block_levels(own_key, shape, cuts, -0.22, 0.18)
    return jnp.clip(array, -most, most).astype(kind)


def setup_inputs(seed: int = 0) -> dict:
    key_of = jax.random.split(jax.random.key(seed), 12)
    return {
        "exposure": gaussian(key_of[0], (CCDS, CROWS, W), 1.0, 6.0, ((0, 16), (1, 2)), jnp.float32),
        "row_shift": place_ends(jax.random.randint(key_of[1], (CCDS,), 0, HALO), jax.random.fold_in(key_of[1], 1), 0, HALO - 1).astype(jnp.int32),
        "row_fraction": jnp.clip(1.0 * jax.random.uniform(key_of[2], (CCDS, CROWS), jnp.float32) ** block_levels(key_of[2], (CCDS, CROWS), ((0, 16), (1, 2)), -0.2, 0.2), 0.0, 1.0).astype(jnp.bfloat16),
        "column_shift": place_ends(jax.random.randint(key_of[3], (CCDS,), 0, PW), jax.random.fold_in(key_of[3], 1), 0, PW - 1).astype(jnp.int32),
        "column_fraction": jnp.clip(1.0 * jax.random.uniform(key_of[4], (CCDS, W), jnp.float32) ** block_levels(key_of[4], (CCDS, W), ((0, 16),), -0.2, 0.2), 0.0, 1.0).astype(jnp.bfloat16),
        "piece_width": place_ends(jax.random.randint(key_of[5], (CCDS, NP), 1, PW + 1), jax.random.fold_in(key_of[5], 1), 1, PW).astype(jnp.int32),
        "route_tile": draw_route_tile(jax.random.fold_in(key_of[11], 71), 0),
        "route_cell": draw_route_cell(jax.random.fold_in(key_of[11], 71), 0),
        "template": gaussian(key_of[8], (NT, CROWS, CAP * PW), 1.0, 6.0, ((0, 16), (1, 2)), jnp.float32),
        "match_kernel": gaussian(key_of[9], (NT, KS, KS), (KS * KS) ** -0.5, 0.15625, ((0, 16),)),
        "detection_kernel": gaussian(key_of[10], (NT, DK, DK), (DK * DK) ** -0.5, 0.375, ((0, 16),)),
    }


def warp_columns(padded, column_offset, fraction):
    length = fraction.shape[-1]
    leftward = lax.dynamic_slice_in_dim(padded, column_offset, length, 1).astype(jnp.float32)
    rightward = lax.dynamic_slice_in_dim(padded, column_offset + 1, length, 1).astype(jnp.float32)
    weight = fraction.astype(jnp.float32)[None, :]
    return (1.0 - weight) * leftward + weight * rightward

def correlate(source, kernel):
    margin = kernel.shape[0] // 2
    output = lax.conv_general_dilated(source[None, None], kernel[None, None], (1, 1), [(margin, margin), (margin, margin)], precision=lax.Precision.HIGHEST)
    return output[0, 0]

def warp_exposure(frame_band, shift_rows, fraction_rows, shift_columns, fraction_columns):
    height = frame_band.shape[0]
    extended = jnp.concatenate([frame_band, jnp.zeros((HALO, frame_band.shape[1]), jnp.float32)], axis=0)
    upper_rows = lax.dynamic_slice_in_dim(extended, shift_rows, height, 0)
    lower_rows = lax.dynamic_slice_in_dim(extended, shift_rows + 1, height, 0)
    weight = fraction_rows.astype(jnp.float32)[:, None]
    warped_rows = ((1.0 - weight) * upper_rows + weight * lower_rows).astype(jnp.bfloat16)
    padded = jnp.pad(warped_rows, ((0, 0), (0, PW)))
    return warp_columns(padded, shift_columns, fraction_columns).astype(jnp.bfloat16)

def match_one(operands):
    return correlate(operands[0].astype(jnp.float32), operands[1].astype(jnp.float32))

def reference(exposure, row_shift, row_fraction, column_shift, column_fraction, piece_width, route_tile, route_cell, template, match_kernel, detection_kernel):
    warped = jax.vmap(warp_exposure)(exposure, row_shift, row_fraction, column_shift, column_fraction)
    lane_index = jnp.arange(PW, dtype=jnp.int32)
    keep_mask = lane_index[None, None, :] < piece_width[:, :, None]
    shaped = warped.reshape(CCDS, CROWS, NP, PW)
    shaped = jnp.where(keep_mask[:, None, :, :], shaped, jnp.zeros((), jnp.bfloat16))
    pieces = shaped.transpose(0, 2, 1, 3).reshape(CCDS * NP, CROWS, PW)
    target = (route_tile * CAP + route_cell).reshape(-1).astype(jnp.int32)
    placed = jnp.zeros((NT * CAP, CROWS, PW), jnp.bfloat16).at[target].set(pieces)
    science = placed.reshape(NT, CAP, CROWS, PW).transpose(0, 2, 1, 3).reshape(NT, CROWS, CAP * PW).astype(jnp.float32)
    cell_width = jnp.zeros((NT * CAP,), jnp.int32).at[target].set(piece_width.reshape(-1).astype(jnp.int32))
    live_mask = (lane_index[None, None, :] < cell_width.reshape(NT, CAP, 1)).reshape(NT, 1, CAP * PW)
    rounded = lax.optimization_barrier(template.astype(jnp.bfloat16))
    matched = lax.map(match_one, (rounded, match_kernel))
    difference = jnp.where(live_mask, science - matched, jnp.zeros((), jnp.float32))
    rounded_difference = lax.optimization_barrier(difference.astype(jnp.bfloat16))
    filtered = lax.map(match_one, (rounded_difference, detection_kernel))
    square_sum = jnp.sum(difference * difference)
    live_count = (CROWS * jnp.sum(cell_width)).astype(jnp.float32)
    noise_level = square_sum / live_count
    detect_weights = detection_kernel.astype(jnp.float32)
    kernel_norm = lax.optimization_barrier(jnp.sum(detect_weights * detect_weights, axis=(1, 2)))
    significance = filtered / jnp.sqrt(1.0 + noise_level * kernel_norm)[:, None, None]
    return (difference, significance, noise_level)
```

```python
import functools

import jax
import jax.numpy as jnp
from jax import lax
from jax.experimental import pallas as pl
from jax.experimental.pallas import tpu as pltpu
from jax.sharding import PartitionSpec as P

PW = 128
PAIR = 2
HALO = 8
SLOT = 32
QUAD = 4
HALF = PW // 2
GROUP = 6
F32 = jnp.float32
BF16 = jnp.bfloat16
MESH = pl.DeviceIdType.MESH


def taps_by_lane(kernel, margin):
    extent = kernel.shape[0]
    b = lax.broadcasted_iota(jnp.int32, (extent, PW), 0)
    lane = lax.broadcasted_iota(jnp.int32, (extent, PW), 1)
    want = margin - b
    want = jnp.where(want < 0, want + PW, want)
    return jnp.dot(kernel, (lane == want).astype(BF16), preferred_element_type=F32)


def build_weights(kernel_ref, taps_ref, taps64_ref, weight_ref):
    extent = kernel_ref.shape[0]
    margin = extent // 2
    taps = taps_by_lane(kernel_ref[...], margin)
    taps_ref[...] = jnp.zeros_like(taps_ref)
    taps64_ref[...] = jnp.zeros_like(taps64_ref)
    taps_ref[8 : 8 + extent, :] = taps
    taps64_ref[8 : 8 + extent, :] = pltpu.roll(taps, HALF, 1)
    lane = lax.broadcasted_iota(jnp.int32, (PW, PW), 1)
    nothing = jnp.zeros((2 * PW, PW), BF16)
    weight_ref[0 : 2 * PW, PW : 2 * PW] = nothing
    weight_ref[(extent + 1) * PW : (extent + 3) * PW, 0:PW] = nothing

    def step(u, carry):
        first = jnp.broadcast_to(taps_ref[pl.ds(u + 8, 1), :], (PW, PW))
        second = jnp.broadcast_to(taps64_ref[pl.ds(u + 7, 1), :], (PW, PW))
        first = pltpu.roll(first, 0, 1, stride=1, stride_axis=0)
        second = pltpu.roll(second, 0, 1, stride=1, stride_axis=0)
        both = jnp.where(lane < HALF, first, second).astype(BF16)
        at = pl.multiple_of(u * PW, PW)
        weight_ref[pl.ds(at, PW), 0:PW] = both
        at = pl.multiple_of((u + 2) * PW, PW)
        weight_ref[pl.ds(at, PW), PW : 2 * PW] = both
        return carry

    lax.fori_loop(0, extent + 1, step, 0)


def build_windows(source_ref, window_ref):
    rows, cells, _ = source_ref.shape

    def step(q, carry):
        x = source_ref[pl.ds(q * QUAD, QUAD)].astype(F32).reshape(QUAD * cells, PW)
        lane = lax.broadcasted_iota(jnp.int32, x.shape, 1)
        cell = lax.broadcasted_iota(jnp.int32, x.shape, 0) % cells
        before = jnp.where(cell == 0, 0.0, pltpu.roll(x, 1, 0))
        after = jnp.where(cell == cells - 1, 0.0, pltpu.roll(x, x.shape[0] - 1, 0))
        even = jnp.where(lane < PW - HALF // 2, x, before)
        odd = pltpu.roll(jnp.where(lane >= HALF // 2, x, after), HALF, 1)
        window_ref[q, :, 0:cells, :] = even.astype(BF16).reshape(QUAD, cells, PW)
        window_ref[q, :, cells : 2 * cells, :] = odd.astype(BF16).reshape(QUAD, cells, PW)
        return carry

    lax.fori_loop(0, rows // QUAD, step, 0)


def run_filter(window_ref, weight_ref, sum_ref, extent, quads):
    reach = extent + QUAD - 1
    blocks = window_ref.shape[2]
    for start in range(0, reach, GROUP):
        stop = min(start + GROUP, reach)
        left = jnp.concatenate(
            [
                window_ref[u // QUAD : u // QUAD + quads, u % QUAD].reshape(quads * blocks, PW)
                for u in range(start, stop)
            ],
            axis=1,
        )
        part = jnp.dot(left, weight_ref[start * PW : stop * PW, :], preferred_element_type=F32)
        if start == 0:
            sum_ref[...] = part
        else:
            sum_ref[...] += part


def filtered_row(sum_ref, row, cells):
    quad, r = divmod(row, QUAD)
    at = quad * 2 * cells
    columns = slice((r // 2) * PW, (r // 2 + 1) * PW)
    even = sum_ref[at : at + cells, columns]
    odd = sum_ref[at + cells : at + 2 * cells, columns]
    lane = lax.broadcasted_iota(jnp.int32, (cells, PW), 1)
    if r % 2 == 0:
        return jnp.where(lane < HALF, even, pltpu.roll(odd, HALF, 1))
    return jnp.where(lane < HALF, pltpu.roll(even, HALF, 1), odd)


def step_kernel(
    n,
    row_shift,
    column_shift,
    piece_width,
    route_tile,
    route_cell,
    exposure,
    row_fraction,
    column_fraction,
    template,
    match_kernel,
    detection_kernel,
    difference,
    significance,
    noise_out,
    extended,
    warped,
    outgoing,
    incoming,
    source,
    window,
    match_weight,
    detect_weight,
    taps,
    taps64,
    total,
    rounded,
    window2,
    partials,
    halo_send,
    halo_recv,
    piece_send,
    piece_recv,
    noise_send,
    noise_recv,
):
    me = lax.axis_index("ccd")
    band = lax.axis_index("row")
    partner = 1 - band
    height, columns = exposure.shape
    pieces = columns // PW
    cells = template.shape[1]
    margin = match_kernel.shape[0] // 2
    margin2 = detection_kernel.shape[0] // 2
    quads = height // QUAD
    everyone = 2 * n

    def peer(index):
        return {
            "ccd": lax.rem(me + lax.rem(index, n), n),
            "row": lax.rem(band + index // n, 2),
        }

    barrier = pltpu.get_barrier_semaphore()

    def greet(index, carry):
        pl.semaphore_signal(barrier, inc=1, device_id=peer(index), device_id_type=MESH)
        return carry

    lax.fori_loop(1, everyone, greet, 0)

    extended[0:height, :] = exposure[...]
    source[margin : margin + height] = template[...]
    outer = jnp.zeros((margin, cells, PW), BF16)
    source[pl.ds(band * (height + margin), margin)] = outer
    rounded[pl.ds(band * (height + margin2), margin2)] = jnp.zeros((margin2, cells, PW), BF16)
    rounded[height + 2 * margin2 :] = jnp.zeros(
        (rounded.shape[0] - height - 2 * margin2, cells, PW), BF16
    )

    pl.semaphore_wait(barrier, everyone - 1)

    exposure_copy = pltpu.make_async_remote_copy(
        src_ref=exposure.at[0:HALO],
        dst_ref=extended.at[height : height + HALO],
        send_sem=halo_send.at[0],
        recv_sem=halo_recv.at[0],
        device_id={"row": partner},
        device_id_type=MESH,
    )
    exposure_copy.start()
    template_copy = pltpu.make_async_remote_copy(
        src_ref=template.at[pl.ds(partner * (height - margin), margin)],
        dst_ref=source.at[pl.ds(band * (height + margin), margin)],
        send_sem=halo_send.at[1],
        recv_sem=halo_recv.at[1],
        device_id={"row": partner},
        device_id_type=MESH,
    )
    template_copy.start()

    build_weights(detection_kernel, taps, taps64, detect_weight)

    exposure_copy.wait()
    below = extended[height : height + HALO, :]
    extended[height : height + HALO, :] = jnp.where(band == 0, below, jnp.zeros_like(below))
    diagonal = lax.broadcasted_iota(jnp.int32, (height, height), 0) == lax.broadcasted_iota(
        jnp.int32, (height, height), 1
    )
    weight = jnp.sum(
        jnp.where(diagonal, jnp.broadcast_to(row_fraction[...].astype(F32), (height, height)), 0.0),
        axis=1,
        keepdims=True,
    )
    shift = row_shift[0]
    slide = column_shift[0]
    lane = lax.broadcasted_iota(jnp.int32, (height, PW), 1)
    all_widths = piece_width[0, 0]
    for p in range(1, pieces):
        all_widths = all_widths + piece_width[0, p]
    meta_row = lax.broadcasted_iota(jnp.int32, (SLOT - height, PW), 0)

    def metadata(cell, width):
        m = jnp.where(meta_row == 0, cell, 0)
        m = jnp.where(meta_row == 1, width, m)
        m = jnp.where(meta_row == 2, all_widths // PW, m)
        m = jnp.where(meta_row == 3, all_widths % PW, m)
        return m.astype(F32)

    rise = height + HALO - shift
    turn1 = lax.rem(PW - slide, PW)
    turn2 = PW - 1 - slide
    after1 = jnp.zeros((height, PW), F32)
    after2 = after1
    warped[pieces] = jnp.concatenate([after1, metadata(-1, 0)], axis=0).astype(BF16)
    for p in reversed(range(pieces)):
        block = slice(p * PW, (p + 1) * PW)
        tall = extended[:, block]
        upper = pltpu.roll(tall, lax.rem(rise, height + HALO), 0)[0:height]
        lower = pltpu.roll(tall, rise - 1, 0)[0:height]
        rows = ((1.0 - weight) * upper + weight * lower).astype(BF16).astype(F32)
        rolled1 = pltpu.roll(rows, turn1, 1)
        rolled2 = pltpu.roll(rows, turn2, 1)
        leftward = jnp.where(lane < PW - slide, rolled1, after1)
        rightward = jnp.where(lane < PW - 1 - slide, rolled2, after2)
        after1, after2 = rolled1, rolled2
        fraction = column_fraction[:, block].astype(F32)
        value = (1.0 - fraction) * leftward + fraction * rightward
        value = jnp.where(lane < piece_width[0, p], value, 0.0)
        warped[p] = jnp.concatenate(
            [value, metadata(route_cell[0, p], piece_width[0, p])], axis=0
        ).astype(BF16)

    def pack(index, carry):
        tile = lax.rem(me + index, n)
        first = pieces
        second = pieces
        for p in reversed(range(pieces)):
            here = route_tile[0, p] == tile
            second = jnp.where(here, first, second)
            first = jnp.where(here, p, first)
        outgoing[index, 0] = warped[first]
        outgoing[index, 1] = warped[second]
        return carry

    lax.fori_loop(0, n, pack, 0)

    def piece_copy(index):
        return pltpu.make_async_remote_copy(
            src_ref=outgoing.at[index],
            dst_ref=incoming.at[index],
            send_sem=piece_send.at[index],
            recv_sem=piece_recv.at[index],
            device_id={"ccd": lax.rem(me + index, n)},
            device_id_type=MESH,
        )

    def send_piece(index, carry):
        piece_copy(index).start()
        return carry

    lax.fori_loop(1, n, send_piece, 0)
    incoming[0] = outgoing[0]

    build_weights(match_kernel, taps, taps64, match_weight)
    template_copy.wait()
    build_windows(source, window)
    run_filter(window, match_weight, total, match_kernel.shape[0], quads)

    def take_piece(index, carry):
        piece_copy(index).wait_recv()
        return carry

    lax.fori_loop(1, n, take_piece, 0)
    chunk = cells // PAIR
    per_vreg = PW // SLOT
    lane_row = lax.broadcasted_iota(jnp.int32, (1, PW), 1)
    cell_of = lax.broadcasted_iota(jnp.int32, (cells, PAIR * chunk * SLOT), 0).astype(F32)
    k_row = lax.broadcasted_iota(jnp.int32, (1, PAIR * chunk * SLOT), 1) % SLOT
    placed_rows = list(range(height)) + [height + 1]
    live_total = jnp.zeros((1, PW), F32)
    placed = None
    for start in range(0, n, chunk):
        meta = [
            incoming[start + s // PAIR, s % PAIR, height : SLOT, :].astype(F32)
            for s in range(PAIR * chunk)
        ]
        for s in range(0, PAIR * chunk, PAIR):
            live_total = live_total + meta[s][2:3] * float(PW) + meta[s][3:4]
        parts = []
        for v in range(PAIR * chunk // per_vreg):
            part = meta[v * per_vreg + per_vreg - 1][0:1]
            for k in reversed(range(per_vreg - 1)):
                part = jnp.where(lane_row < (k + 1) * SLOT, meta[v * per_vreg + k][0:1], part)
            parts.append(part)
        cell_row = jnp.concatenate(parts, axis=1)
        placer = jnp.concatenate(
            [
                jnp.where(jnp.where(k_row == r, cell_row, -1.0) == cell_of, 1.0, 0.0).astype(BF16)
                for r in placed_rows
            ],
            axis=0,
        )
        block = incoming[start : start + chunk].reshape(PAIR * chunk * SLOT, PW)
        got = jnp.dot(placer, block, preferred_element_type=F32)
        placed = got if placed is None else placed + got
    width_of = placed[height * cells : (height + 1) * cells]
    live = lax.broadcasted_iota(jnp.int32, (cells, PW), 1).astype(F32) < width_of
    squares = jnp.zeros((cells, PW), F32)
    for r in range(height):
        d = placed[r * cells : (r + 1) * cells] - filtered_row(total, r, cells)
        d = jnp.where(live, d, 0.0)
        difference[r] = d
        squares = squares + d * d
        rounded[margin2 + r] = d.astype(BF16)
    partials[0] = jnp.sum(squares.reshape(cells // 8, 8, PW), axis=0)

    difference_copy = pltpu.make_async_remote_copy(
        src_ref=rounded.at[pl.ds(margin2 + partner * (height - margin2), margin2)],
        dst_ref=rounded.at[pl.ds(band * (height + margin2), margin2)],
        send_sem=halo_send.at[2],
        recv_sem=halo_recv.at[2],
        device_id={"row": partner},
        device_id_type=MESH,
    )
    difference_copy.start()

    def noise_copy(index):
        return pltpu.make_async_remote_copy(
            src_ref=partials.at[0],
            dst_ref=partials.at[index],
            send_sem=noise_send.at[index],
            recv_sem=noise_recv.at[index],
            device_id=peer(index),
            device_id_type=MESH,
        )

    def send_noise(index, carry):
        noise_copy(index).start()
        return carry

    lax.fori_loop(1, everyone, send_noise, 0)

    difference_copy.wait()
    build_windows(rounded, window2)
    run_filter(window2, detect_weight, total, detection_kernel.shape[0], quads)

    def take_noise(index, carry):
        noise_copy(index).wait()
        return carry

    lax.fori_loop(1, everyone, take_noise, 0)

    def end_piece(index, carry):
        piece_copy(index).wait_send()
        return carry

    lax.fori_loop(1, n, end_piece, 0)

    squares = jnp.sum(partials[...], axis=0)
    square_sum = jnp.sum(jnp.sum(squares, axis=0, keepdims=True), axis=1, keepdims=True)
    live_count = live_total[:, 0:1] * float(2 * height)
    noise = square_sum / live_count
    detect = detection_kernel[...].astype(F32)
    norm = jnp.sum(jnp.sum(detect * detect, axis=0, keepdims=True), axis=1, keepdims=True)
    scale = 1.0 / jnp.sqrt(1.0 + noise * norm)
    scale = jnp.broadcast_to(scale, (cells, PW))
    for r in range(height):
        significance[r] = filtered_row(total, r, cells) * scale
    noise_out[...] = jnp.broadcast_to(noise, noise_out.shape)


def on_device(
    n,
    exposure,
    row_shift,
    row_fraction,
    column_shift,
    column_fraction,
    piece_width,
    route_tile,
    route_cell,
    template,
    match_kernel,
    detection_kernel,
):
    height, columns = exposure.shape[1:]
    pieces = columns // PW
    cells = template.shape[2] // PW
    extent = match_kernel.shape[1]
    extent2 = detection_kernel.shape[1]
    rows = height + 2 * (extent // 2)
    rows2 = -(-(height + 2 * (extent2 // 2)) // QUAD) * QUAD
    smem = pl.BlockSpec(memory_space=pltpu.SMEM)
    vmem = pl.BlockSpec(memory_space=pltpu.VMEM)
    tiles = template[0].astype(BF16).reshape(height, cells, PW)
    difference, significance, noise = pl.pallas_call(
        functools.partial(step_kernel, n),
        out_shape=(
            jax.ShapeDtypeStruct((height, cells, PW), F32),
            jax.ShapeDtypeStruct((height, cells, PW), F32),
            jax.ShapeDtypeStruct((8, PW), F32),
        ),
        in_specs=[smem] * 5 + [vmem] * 6,
        out_specs=(vmem, vmem, vmem),
        scratch_shapes=[
            pltpu.VMEM((height + HALO, columns), F32),
            pltpu.VMEM((pieces + 1, SLOT, PW), BF16),
            pltpu.VMEM((n, PAIR, SLOT, PW), BF16),
            pltpu.VMEM((n, PAIR, SLOT, PW), BF16),
            pltpu.VMEM((rows, cells, PW), BF16),
            pltpu.VMEM((rows // QUAD, QUAD, 2 * cells, PW), BF16),
            pltpu.VMEM(((extent + QUAD - 1) * PW, 2 * PW), BF16),
            pltpu.VMEM(((extent2 + QUAD - 1) * PW, 2 * PW), BF16),
            pltpu.VMEM((extent + 15, PW), F32),
            pltpu.VMEM((extent + 15, PW), F32),
            pltpu.VMEM((height // QUAD * 2 * cells, 2 * PW), F32),
            pltpu.VMEM((rows2, cells, PW), BF16),
            pltpu.VMEM((rows2 // QUAD, QUAD, 2 * cells, PW), BF16),
            pltpu.VMEM((2 * n, 8, PW), F32),
            pltpu.SemaphoreType.DMA((3,)),
            pltpu.SemaphoreType.DMA((3,)),
            pltpu.SemaphoreType.DMA((n,)),
            pltpu.SemaphoreType.DMA((n,)),
            pltpu.SemaphoreType.DMA((2 * n,)),
            pltpu.SemaphoreType.DMA((2 * n,)),
        ],
        compiler_params=pltpu.CompilerParams(
            collective_id=0, has_side_effects=True, vmem_limit_bytes=40 * 2**20
        ),
    )(
        row_shift,
        column_shift,
        piece_width,
        route_tile,
        route_cell,
        exposure[0],
        row_fraction,
        column_fraction,
        tiles,
        match_kernel[0],
        detection_kernel[0],
    )
    shape = (1, height, cells * PW)
    return (difference.reshape(shape), significance.reshape(shape), noise[0, 0])


def solution(mesh):
    assert mesh.shape["row"] == 2
    return jax.shard_map(
        functools.partial(on_device, mesh.shape["ccd"]),
        mesh=mesh,
        in_specs=(
            P("ccd", "row", None),
            P("ccd"),
            P("ccd", "row"),
            P("ccd"),
            P("ccd", None),
            P("ccd", None),
            P("ccd", None),
            P("ccd", None),
            P("ccd", "row", None),
            P("ccd", None, None),
            P("ccd", None, None),
        ),
        out_specs=(P("ccd", "row", None), P("ccd", "row", None), P()),
        check_vma=False,
    )
```

```python
import functools

import jax
import jax.numpy as jnp
from jax import lax
from jax.experimental import pallas as pl
from jax.experimental.pallas import tpu as pltpu
from jax.sharding import PartitionSpec as P

PW = 128
PAIR = 2
HALO = 8
SLOT = 32
QUAD = 4
HALF = PW // 2
GROUP = 6
F32 = jnp.float32
BF16 = jnp.bfloat16
MESH = pl.DeviceIdType.MESH


def taps_by_lane(kernel, margin):
    extent = kernel.shape[0]
    b = lax.broadcasted_iota(jnp.int32, (extent, PW), 0)
    lane = lax.broadcasted_iota(jnp.int32, (extent, PW), 1)
    want = margin - b
    want = jnp.where(want < 0, want + PW, want)
    return jnp.dot(kernel, (lane == want).astype(BF16), preferred_element_type=F32)


def build_weights(kernel_ref, taps_ref, taps64_ref, weight_ref):
    extent = kernel_ref.shape[0]
    margin = extent // 2
    taps = taps_by_lane(kernel_ref[...], margin)
    taps_ref[...] = jnp.zeros_like(taps_ref)
    taps64_ref[...] = jnp.zeros_like(taps64_ref)
    taps_ref[8 : 8 + extent, :] = taps
    taps64_ref[8 : 8 + extent, :] = pltpu.roll(taps, HALF, 1)
    lane = lax.broadcasted_iota(jnp.int32, (PW, PW), 1)
    nothing = jnp.zeros((2 * PW, PW), BF16)
    weight_ref[0 : 2 * PW, PW : 2 * PW] = nothing
    weight_ref[(extent + 1) * PW : (extent + 3) * PW, 0:PW] = nothing

    def step(u, carry):
        first = jnp.broadcast_to(taps_ref[pl.ds(u + 8, 1), :], (PW, PW))
        second = jnp.broadcast_to(taps64_ref[pl.ds(u + 7, 1), :], (PW, PW))
        first = pltpu.roll(first, 0, 1, stride=1, stride_axis=0)
        second = pltpu.roll(second, 0, 1, stride=1, stride_axis=0)
        both = jnp.where(lane < HALF, first, second).astype(BF16)
        at = pl.multiple_of(u * PW, PW)
        weight_ref[pl.ds(at, PW), 0:PW] = both
        at = pl.multiple_of((u + 2) * PW, PW)
        weight_ref[pl.ds(at, PW), PW : 2 * PW] = both
        return carry

    lax.fori_loop(0, extent + 1, step, 0)


def build_windows(source_ref, window_ref, first, count):
    rows, cells, _ = source_ref.shape

    def step(index, carry):
        q = first + index
        x = source_ref[pl.ds(q * QUAD, QUAD)].astype(F32).reshape(QUAD * cells, PW)
        lane = lax.broadcasted_iota(jnp.int32, x.shape, 1)
        cell = lax.broadcasted_iota(jnp.int32, x.shape, 0) % cells
        before = jnp.where(cell == 0, 0.0, pltpu.roll(x, 1, 0))
        after = jnp.where(cell == cells - 1, 0.0, pltpu.roll(x, x.shape[0] - 1, 0))
        even = jnp.where(lane < PW - HALF // 2, x, before)
        odd = pltpu.roll(jnp.where(lane >= HALF // 2, x, after), HALF, 1)
        window_ref[q, :, 0:cells, :] = even.astype(BF16).reshape(QUAD, cells, PW)
        window_ref[q, :, cells : 2 * cells, :] = odd.astype(BF16).reshape(QUAD, cells, PW)
        return carry

    lax.fori_loop(0, count, step, 0)


def run_filter(window_ref, weight_ref, sum_ref, extent, quads, skip):
    reach = extent + QUAD - 1
    blocks = window_ref.shape[2]
    for start in range(0, reach, GROUP):
        stop = min(start + GROUP, reach)
        left = jnp.concatenate(
            [
                window_ref[(u + skip) // QUAD : (u + skip) // QUAD + quads, (u + skip) % QUAD].reshape(quads * blocks, PW)
                for u in range(start, stop)
            ],
            axis=1,
        )
        part = jnp.dot(left, weight_ref[start * PW : stop * PW, :], preferred_element_type=F32)
        if start == 0:
            sum_ref[...] = part
        else:
            sum_ref[...] += part


def filtered_row(sum_ref, row, cells):
    quad, r = divmod(row, QUAD)
    at = quad * 2 * cells
    columns = slice((r // 2) * PW, (r // 2 + 1) * PW)
    even = sum_ref[at : at + cells, columns]
    odd = sum_ref[at + cells : at + 2 * cells, columns]
    lane = lax.broadcasted_iota(jnp.int32, (cells, PW), 1)
    if r % 2 == 0:
        return jnp.where(lane < HALF, even, pltpu.roll(odd, HALF, 1))
    return jnp.where(lane < HALF, pltpu.roll(even, HALF, 1), odd)


def step_kernel(
    n,
    row_shift,
    column_shift,
    piece_width,
    route_tile,
    route_cell,
    exposure,
    row_fraction,
    column_fraction,
    template,
    match_kernel,
    detection_kernel,
    difference,
    significance,
    noise_out,
    extended,
    warped,
    outgoing,
    incoming,
    tiles,
    source,
    window,
    match_weight,
    detect_weight,
    taps,
    taps64,
    total,
    rounded,
    window2,
    partials,
    halo_send,
    halo_recv,
    piece_send,
    piece_recv,
    noise_send,
    noise_recv,
):
    me = lax.axis_index("ccd")
    band = lax.axis_index("row")
    partner = 1 - band
    height, columns = exposure.shape
    pieces = columns // PW
    cells = template.shape[0] // height
    margin = match_kernel.shape[0] // 2
    margin2 = detection_kernel.shape[0] // 2
    quads = height // QUAD
    everyone = 2 * n
    rows2 = rounded.shape[0]
    lead = rows2 // 2 - height // 2

    def peer(index):
        other = index >= n
        at = me + jnp.where(other, index - n, index)
        return {
            "ccd": jnp.where(at >= n, at - n, at),
            "row": jnp.where(other, partner, band),
        }

    def along(index):
        at = me + index
        return jnp.where(at >= n, at - n, at)

    barrier = pltpu.get_barrier_semaphore()

    def greet(index, carry):
        pl.semaphore_signal(barrier, inc=1, device_id=peer(index), device_id_type=MESH)
        return carry

    lax.fori_loop(1, everyone, greet, 0)

    extended[0:height, :] = exposure[...]
    outer = jnp.zeros((margin, cells, PW), BF16)
    source[pl.ds(band * (height + margin), margin)] = outer
    for r in range(height):
        tiles[r] = template[pl.ds(r // 8 * cells * 8 + r % 8, cells, stride=8), :].astype(BF16)
    source[margin : margin + height] = tiles[...]
    for q in (0, 1, rows2 // QUAD - 2, rows2 // QUAD - 1):
        rounded[q * QUAD : (q + 1) * QUAD] = jnp.zeros((QUAD, cells, PW), BF16)
    build_weights(detection_kernel, taps, taps64, detect_weight)
    build_weights(match_kernel, taps, taps64, match_weight)
    build_windows(source, window, margin // QUAD, quads)
    build_windows(source, window, band * ((height + margin) // QUAD), margin // QUAD)

    pl.semaphore_wait(barrier, everyone - 1)

    exposure_copy = pltpu.make_async_remote_copy(
        src_ref=exposure.at[0:HALO],
        dst_ref=extended.at[height : height + HALO],
        send_sem=halo_send.at[0],
        recv_sem=halo_recv.at[0],
        device_id={"row": partner},
        device_id_type=MESH,
    )
    exposure_copy.start()
    template_copy = pltpu.make_async_remote_copy(
        src_ref=tiles.at[pl.ds(partner * (height - margin), margin)],
        dst_ref=source.at[pl.ds(band * (height + margin), margin)],
        send_sem=halo_send.at[1],
        recv_sem=halo_recv.at[1],
        device_id={"row": partner},
        device_id_type=MESH,
    )
    template_copy.start()

    exposure_copy.wait()
    below = extended[height : height + HALO, :]
    extended[height : height + HALO, :] = jnp.where(band == 0, below, jnp.zeros_like(below))
    diagonal = lax.broadcasted_iota(jnp.int32, (height, height), 0) == lax.broadcasted_iota(
        jnp.int32, (height, height), 1
    )
    weight = jnp.sum(
        jnp.where(diagonal, jnp.broadcast_to(row_fraction[...].astype(F32), (height, height)), 0.0),
        axis=1,
        keepdims=True,
    )
    shift = row_shift[0]
    slide = column_shift[0]
    lane = lax.broadcasted_iota(jnp.int32, (height, PW), 1)
    all_widths = piece_width[0, 0]
    for p in range(1, pieces):
        all_widths = all_widths + piece_width[0, p]
    meta_row = lax.broadcasted_iota(jnp.int32, (SLOT - height, PW), 0)

    def metadata(cell, width):
        m = jnp.where(meta_row == 0, cell, 0)
        m = jnp.where(meta_row == 1, width, m)
        m = jnp.where(meta_row == 2, all_widths // PW, m)
        m = jnp.where(meta_row == 3, all_widths % PW, m)
        return m.astype(F32)

    rise = height + HALO - shift
    turn1 = lax.rem(PW - slide, PW)
    turn2 = PW - 1 - slide
    after1 = jnp.zeros((height, PW), F32)
    after2 = after1
    warped[pieces] = jnp.concatenate([after1, metadata(-1, 0)], axis=0).astype(BF16)
    for p in reversed(range(pieces)):
        block = slice(p * PW, (p + 1) * PW)
        tall = extended[:, block]
        upper = pltpu.roll(tall, lax.rem(rise, height + HALO), 0)[0:height]
        lower = pltpu.roll(tall, rise - 1, 0)[0:height]
        rows = ((1.0 - weight) * upper + weight * lower).astype(BF16).astype(F32)
        rolled1 = pltpu.roll(rows, turn1, 1)
        rolled2 = pltpu.roll(rows, turn2, 1)
        leftward = jnp.where(lane < PW - slide, rolled1, after1)
        rightward = jnp.where(lane < PW - 1 - slide, rolled2, after2)
        after1, after2 = rolled1, rolled2
        fraction = column_fraction[:, block].astype(F32)
        value = (1.0 - fraction) * leftward + fraction * rightward
        value = jnp.where(lane < piece_width[0, p], value, 0.0)
        warped[p] = jnp.concatenate(
            [value, metadata(route_cell[0, p], piece_width[0, p])], axis=0
        ).astype(BF16)

    def pack(index, carry):
        tile = along(index)
        first = pieces
        second = pieces
        for p in reversed(range(pieces)):
            here = route_tile[0, p] == tile
            second = jnp.where(here, first, second)
            first = jnp.where(here, p, first)
        outgoing[index, 0] = warped[first]
        outgoing[index, 1] = warped[second]
        return carry

    lax.fori_loop(0, n, pack, 0)

    def piece_copy(index):
        return pltpu.make_async_remote_copy(
            src_ref=outgoing.at[index],
            dst_ref=incoming.at[index],
            send_sem=piece_send.at[index],
            recv_sem=piece_recv.at[index],
            device_id={"ccd": along(index)},
            device_id_type=MESH,
        )

    def send_piece(index, carry):
        piece_copy(index).start()
        return carry

    lax.fori_loop(1, n, send_piece, 0)
    incoming[0] = outgoing[0]

    template_copy.wait()
    build_windows(source, window, partner * ((height + margin) // QUAD), margin // QUAD)
    run_filter(window, match_weight, total, match_kernel.shape[0], quads, 0)

    def take_piece(index, carry):
        piece_copy(index).wait_recv()
        return carry

    lax.fori_loop(1, n, take_piece, 0)
    chunk = cells // PAIR
    per_vreg = PW // SLOT
    lane_row = lax.broadcasted_iota(jnp.int32, (1, PW), 1)
    cell_of = lax.broadcasted_iota(jnp.int32, (cells, PAIR * chunk * SLOT), 0).astype(F32)
    k_row = lax.broadcasted_iota(jnp.int32, (1, PAIR * chunk * SLOT), 1) % SLOT
    placed_rows = list(range(height)) + [height + 1]
    live_total = jnp.zeros((1, PW), F32)
    placed = None
    for start in range(0, n, chunk):
        meta = [
            incoming[start + s // PAIR, s % PAIR, height : SLOT, :].astype(F32)
            for s in range(PAIR * chunk)
        ]
        for s in range(0, PAIR * chunk, PAIR):
            live_total = live_total + meta[s][2:3] * float(PW) + meta[s][3:4]
        parts = []
        for v in range(PAIR * chunk // per_vreg):
            part = meta[v * per_vreg + per_vreg - 1][0:1]
            for k in reversed(range(per_vreg - 1)):
                part = jnp.where(lane_row < (k + 1) * SLOT, meta[v * per_vreg + k][0:1], part)
            parts.append(part)
        cell_row = jnp.concatenate(parts, axis=1)
        placer = jnp.concatenate(
            [
                jnp.where(jnp.where(k_row == r, cell_row, -1.0) == cell_of, 1.0, 0.0).astype(BF16)
                for r in placed_rows
            ],
            axis=0,
        )
        block = incoming[start : start + chunk].reshape(PAIR * chunk * SLOT, PW)
        got = jnp.dot(placer, block, preferred_element_type=F32)
        placed = got if placed is None else placed + got
    width_of = placed[height * cells : (height + 1) * cells]
    live = lax.broadcasted_iota(jnp.int32, (cells, PW), 1).astype(F32) < width_of
    squares = jnp.zeros((cells, PW), F32)
    for r in range(height):
        d = placed[r * cells : (r + 1) * cells] - filtered_row(total, r, cells)
        d = jnp.where(live, d, 0.0)
        difference[pl.ds(r // 8 * cells * 8 + r % 8, cells, stride=8), :] = d
        squares = squares + d * d
        rounded[lead + r] = d.astype(BF16)
    partials[0] = jnp.sum(squares.reshape(cells // 8, 8, PW), axis=0)

    difference_copy = pltpu.make_async_remote_copy(
        src_ref=rounded.at[pl.ds(lead + partner * (height - margin2), margin2)],
        dst_ref=rounded.at[pl.ds(lead - margin2 + band * (height + margin2), margin2)],
        send_sem=halo_send.at[2],
        recv_sem=halo_recv.at[2],
        device_id={"row": partner},
        device_id_type=MESH,
    )
    difference_copy.start()

    def noise_copy(index):
        return pltpu.make_async_remote_copy(
            src_ref=partials.at[0],
            dst_ref=partials.at[index],
            send_sem=noise_send.at[index],
            recv_sem=noise_recv.at[index],
            device_id=peer(index),
            device_id_type=MESH,
        )

    def send_noise(index, carry):
        noise_copy(index).start()
        return carry

    lax.fori_loop(1, everyone, send_noise, 0)

    build_windows(rounded, window2, lead // QUAD, quads)
    build_windows(rounded, window2, band * ((height + lead) // QUAD), lead // QUAD)
    difference_copy.wait()
    build_windows(rounded, window2, partner * ((height + lead) // QUAD), lead // QUAD)
    run_filter(window2, detect_weight, total, detection_kernel.shape[0], quads, lead - margin2)

    def take_noise(index, carry):
        noise_copy(index).wait()
        return carry

    lax.fori_loop(1, everyone, take_noise, 0)

    def end_piece(index, carry):
        piece_copy(index).wait_send()
        return carry

    lax.fori_loop(1, n, end_piece, 0)

    squares = jnp.sum(partials[...], axis=0)
    square_sum = jnp.sum(jnp.sum(squares, axis=0, keepdims=True), axis=1, keepdims=True)
    live_count = live_total[:, 0:1] * float(2 * height)
    noise = square_sum / live_count
    detect = detection_kernel[...].astype(F32)
    norm = jnp.sum(jnp.sum(detect * detect, axis=0, keepdims=True), axis=1, keepdims=True)
    scale = 1.0 / jnp.sqrt(1.0 + noise * norm)
    scale = jnp.broadcast_to(scale, (cells, PW))
    for r in range(height):
        significance[pl.ds(r // 8 * cells * 8 + r % 8, cells, stride=8), :] = (
            filtered_row(total, r, cells) * scale
        )
    noise_out[...] = noise


def on_device(
    n,
    exposure,
    row_shift,
    row_fraction,
    column_shift,
    column_fraction,
    piece_width,
    route_tile,
    route_cell,
    template,
    match_kernel,
    detection_kernel,
):
    height, columns = exposure.shape[1:]
    pieces = columns // PW
    cells = template.shape[2] // PW
    extent = match_kernel.shape[1]
    extent2 = detection_kernel.shape[1]
    rows = height + 2 * (extent // 2)
    rows2 = height + 2 * QUAD * -(-(extent2 // 2) // QUAD)
    smem = pl.BlockSpec(memory_space=pltpu.SMEM)
    vmem = pl.BlockSpec(memory_space=pltpu.VMEM)
    tiles = template.reshape(height // 8, 8, cells, PW).transpose(0, 2, 1, 3).reshape(height * cells, PW)
    difference, significance, noise = pl.pallas_call(
        functools.partial(step_kernel, n),
        out_shape=(
            jax.ShapeDtypeStruct((height * cells, PW), F32),
            jax.ShapeDtypeStruct((height * cells, PW), F32),
            jax.ShapeDtypeStruct((1, 1), F32),
        ),
        in_specs=[smem] * 5 + [vmem] * 6,
        out_specs=(vmem, vmem, vmem),
        scratch_shapes=[
            pltpu.VMEM((height + HALO, columns), F32),
            pltpu.VMEM((pieces + 1, SLOT, PW), BF16),
            pltpu.VMEM((n, PAIR, SLOT, PW), BF16),
            pltpu.VMEM((n, PAIR, SLOT, PW), BF16),
            pltpu.VMEM((height, cells, PW), BF16),
            pltpu.VMEM((rows, cells, PW), BF16),
            pltpu.VMEM((rows // QUAD, QUAD, 2 * cells, PW), BF16),
            pltpu.VMEM(((extent + QUAD - 1) * PW, 2 * PW), BF16),
            pltpu.VMEM(((extent2 + QUAD - 1) * PW, 2 * PW), BF16),
            pltpu.VMEM((extent + 15, PW), F32),
            pltpu.VMEM((extent + 15, PW), F32),
            pltpu.VMEM((height // QUAD * 2 * cells, 2 * PW), F32),
            pltpu.VMEM((rows2, cells, PW), BF16),
            pltpu.VMEM((rows2 // QUAD, QUAD, 2 * cells, PW), BF16),
            pltpu.VMEM((2 * n, 8, PW), F32),
            pltpu.SemaphoreType.DMA((3,)),
            pltpu.SemaphoreType.DMA((3,)),
            pltpu.SemaphoreType.DMA((n,)),
            pltpu.SemaphoreType.DMA((n,)),
            pltpu.SemaphoreType.DMA((2 * n,)),
            pltpu.SemaphoreType.DMA((2 * n,)),
        ],
        compiler_params=pltpu.CompilerParams(
            collective_id=0, has_side_effects=True, vmem_limit_bytes=40 * 2**20
        ),
    )(
        row_shift,
        column_shift,
        piece_width,
        route_tile,
        route_cell,
        exposure[0],
        row_fraction,
        column_fraction,
        tiles,
        match_kernel[0],
        detection_kernel[0],
    )

    def as_rows(x):
        x = x.reshape(height // 8, cells, 8, PW).transpose(0, 2, 1, 3)
        return x.reshape(1, height, cells * PW)

    return (as_rows(difference), as_rows(significance), noise.reshape(()))


def solution(mesh):
    assert mesh.shape["row"] == 2
    return jax.shard_map(
        functools.partial(on_device, mesh.shape["ccd"]),
        mesh=mesh,
        in_specs=(
            P("ccd", "row", None),
            P("ccd"),
            P("ccd", "row"),
            P("ccd"),
            P("ccd", None),
            P("ccd", None),
            P("ccd", None),
            P("ccd", None),
            P("ccd", "row", None),
            P("ccd", None, None),
            P("ccd", None, None),
        ),
        out_specs=(P("ccd", "row", None), P("ccd", "row", None), P()),
        check_vma=False,
    )
```

```python
import functools

import jax
import jax.numpy as jnp
from jax import lax
from jax.experimental import pallas as pl
from jax.experimental.pallas import tpu as pltpu
from jax.sharding import PartitionSpec as P

PW = 128
PAIR = 2
HALO = 8
SLOT = 32
QUAD = 4
HALF = PW // 2
GROUP = 6
F32 = jnp.float32
BF16 = jnp.bfloat16
MESH = pl.DeviceIdType.MESH


def taps_by_lane(kernel, margin):
    extent = kernel.shape[0]
    b = lax.broadcasted_iota(jnp.int32, (extent, PW), 0)
    lane = lax.broadcasted_iota(jnp.int32, (extent, PW), 1)
    want = margin - b
    want = jnp.where(want < 0, want + PW, want)
    return jnp.dot(kernel, (lane == want).astype(BF16), preferred_element_type=F32)


def build_weights(kernel_ref, taps_ref, weight_ref):
    extent = kernel_ref.shape[0]
    margin = extent // 2
    taps_ref[...] = jnp.zeros_like(taps_ref)
    taps_ref[8 : 8 + extent, :] = taps_by_lane(kernel_ref[...], margin)
    lane = lax.broadcasted_iota(jnp.int32, (PW, PW), 1)
    nothing = jnp.zeros((2 * PW, PW), BF16)
    weight_ref[0 : 2 * PW, PW : 2 * PW] = nothing
    weight_ref[(extent + 1) * PW : (extent + 3) * PW, 0:PW] = nothing

    def circulant(u):
        row = jnp.broadcast_to(taps_ref[pl.ds(u + 8, 1), :], (PW, PW))
        return pltpu.roll(row, 0, 1, stride=1, stride_axis=0)

    def place(u, first, second):
        second = jnp.concatenate([second[HALF:], second[:HALF]], axis=0)
        both = jnp.where(lane < HALF, first, second).astype(BF16)
        at = pl.multiple_of(u * PW, PW)
        weight_ref[pl.ds(at, PW), 0:PW] = both
        at = pl.multiple_of((u + 2) * PW, PW)
        weight_ref[pl.ds(at, PW), PW : 2 * PW] = both

    def step(index, before):
        u = 2 * index
        now = circulant(u)
        after = circulant(u + 1)
        place(u, now, before)
        place(u + 1, after, now)
        return after

    lax.fori_loop(0, (extent + 1) // 2, step, jnp.zeros((PW, PW), F32))


def build_windows(source_ref, window_ref, first, count):
    rows, cells, _ = source_ref.shape

    def step(index, carry):
        q = first + index
        x = source_ref[pl.ds(q * QUAD, QUAD)].astype(F32).reshape(QUAD * cells, PW)
        lane = lax.broadcasted_iota(jnp.int32, x.shape, 1)
        cell = lax.broadcasted_iota(jnp.int32, x.shape, 0) % cells
        before = jnp.where(cell == 0, 0.0, pltpu.roll(x, 1, 0))
        after = jnp.where(cell == cells - 1, 0.0, pltpu.roll(x, x.shape[0] - 1, 0))
        even = jnp.where(lane < PW - HALF // 2, x, before)
        odd = pltpu.roll(jnp.where(lane >= HALF // 2, x, after), HALF, 1)
        window_ref[q, :, 0:cells, :] = even.astype(BF16).reshape(QUAD, cells, PW)
        window_ref[q, :, cells : 2 * cells, :] = odd.astype(BF16).reshape(QUAD, cells, PW)
        return carry

    lax.fori_loop(0, count, step, 0)


def run_filter(window_ref, weight_ref, sum_ref, extent, quads, skip):
    reach = extent + QUAD - 1
    blocks = window_ref.shape[2]
    for start in range(0, reach, GROUP):
        stop = min(start + GROUP, reach)
        left = jnp.concatenate(
            [
                window_ref[(u + skip) // QUAD : (u + skip) // QUAD + quads, (u + skip) % QUAD].reshape(quads * blocks, PW)
                for u in range(start, stop)
            ],
            axis=1,
        )
        part = jnp.dot(left, weight_ref[start * PW : stop * PW, :], preferred_element_type=F32)
        if start == 0:
            sum_ref[...] = part
        else:
            sum_ref[...] += part


def filtered_row(sum_ref, row, cells):
    quad, r = divmod(row, QUAD)
    at = quad * 2 * cells
    columns = slice((r // 2) * PW, (r // 2 + 1) * PW)
    even = sum_ref[at : at + cells, columns]
    odd = sum_ref[at + cells : at + 2 * cells, columns]
    lane = lax.broadcasted_iota(jnp.int32, (cells, PW), 1)
    if r % 2 == 0:
        return jnp.where(lane < HALF, even, pltpu.roll(odd, HALF, 1))
    return jnp.where(lane < HALF, pltpu.roll(even, HALF, 1), odd)


def step_kernel(
    n,
    row_shift_hbm,
    column_shift_hbm,
    piece_width_hbm,
    route_tile_hbm,
    route_cell_hbm,
    exposure_hbm,
    row_fraction_hbm,
    column_fraction_hbm,
    template_hbm,
    match_kernel_hbm,
    detection_kernel_hbm,
    difference,
    significance,
    noise_out,
    row_shift,
    column_shift,
    piece_width,
    route_tile,
    route_cell,
    row_fraction,
    column_fraction,
    template,
    match_kernel,
    detection_kernel,
    chosen,
    extended,
    warped,
    outgoing,
    incoming,
    tiles,
    source,
    window,
    match_weight,
    detect_weight,
    taps,
    total,
    rounded,
    window2,
    partials,
    load_sem,
    halo_send,
    halo_recv,
    piece_send,
    piece_recv,
    noise_send,
    noise_recv,
):
    height, columns = exposure_hbm.shape
    loads = [
        pltpu.make_async_copy(a, b, load_sem.at[k])
        for k, (a, b) in enumerate(
            [
                (exposure_hbm, extended.at[0:height]),
                (route_tile_hbm, route_tile),
                (route_cell_hbm, route_cell),
                (piece_width_hbm, piece_width),
                (row_shift_hbm, row_shift),
                (column_shift_hbm, column_shift),
                (row_fraction_hbm, row_fraction),
                (column_fraction_hbm, column_fraction),
                (template_hbm, template),
                (match_kernel_hbm, match_kernel),
                (detection_kernel_hbm, detection_kernel),
            ]
        )
    ]
    for load in loads:
        load.start()
    me = lax.axis_index("ccd")
    band = lax.axis_index("row")
    partner = 1 - band
    pieces = columns // PW
    cells = template.shape[0] // height
    margin = match_kernel.shape[0] // 2
    margin2 = detection_kernel.shape[0] // 2
    quads = height // QUAD
    everyone = 2 * n
    rows2 = rounded.shape[0]
    lead = rows2 // 2 - height // 2

    def peer(index):
        other = index >= n
        at = me + jnp.where(other, index - n, index)
        return {
            "ccd": jnp.where(at >= n, at - n, at),
            "row": jnp.where(other, partner, band),
        }

    def along(index):
        at = me + index
        return jnp.where(at >= n, at - n, at)

    barrier = pltpu.get_barrier_semaphore()

    def greet(index, carry):
        pl.semaphore_signal(barrier, inc=1, device_id=peer(index), device_id_type=MESH)
        return carry

    lax.fori_loop(1, everyone, greet, 0)

    outer = jnp.zeros((margin, cells, PW), BF16)
    source[pl.ds(band * (height + margin), margin)] = outer
    for q in (0, 1, rows2 // QUAD - 2, rows2 // QUAD - 1):
        rounded[q * QUAD : (q + 1) * QUAD] = jnp.zeros((QUAD, cells, PW), BF16)
    loads[0].wait()
    pl.semaphore_wait(barrier, everyone - 1)

    exposure_copy = pltpu.make_async_remote_copy(
        src_ref=extended.at[0:HALO],
        dst_ref=extended.at[height : height + HALO],
        send_sem=halo_send.at[0],
        recv_sem=halo_recv.at[0],
        device_id={"row": partner},
        device_id_type=MESH,
    )
    exposure_copy.start()
    for load in loads[1:8]:
        load.wait()

    def choose(index, carry):
        tile = along(index)
        first = pieces
        second = pieces
        for p in reversed(range(pieces)):
            here = route_tile[0, p] == tile
            second = jnp.where(here, first, second)
            first = jnp.where(here, p, first)
        chosen[index, 0] = first
        chosen[index, 1] = second
        return carry

    lax.fori_loop(0, n, choose, 0)

    exposure_copy.wait()
    below = extended[height : height + HALO, :]
    extended[height : height + HALO, :] = jnp.where(band == 0, below, jnp.zeros_like(below))
    diagonal = lax.broadcasted_iota(jnp.int32, (height, height), 0) == lax.broadcasted_iota(
        jnp.int32, (height, height), 1
    )
    weight = jnp.sum(
        jnp.where(diagonal, jnp.broadcast_to(row_fraction[...].astype(F32), (height, height)), 0.0),
        axis=1,
        keepdims=True,
    )
    shift = row_shift[0]
    slide = column_shift[0]
    lane = lax.broadcasted_iota(jnp.int32, (height, PW), 1)
    all_widths = piece_width[0, 0]
    for p in range(1, pieces):
        all_widths = all_widths + piece_width[0, p]
    meta_row = lax.broadcasted_iota(jnp.int32, (SLOT - height, PW), 0)

    def metadata(cell, width):
        m = jnp.where(meta_row == 0, cell, 0)
        m = jnp.where(meta_row == 1, width, m)
        m = jnp.where(meta_row == 2, all_widths // PW, m)
        m = jnp.where(meta_row == 3, all_widths % PW, m)
        return m.astype(F32)

    rise = height + HALO - shift
    turn1 = lax.rem(PW - slide, PW)
    turn2 = PW - 1 - slide
    after1 = jnp.zeros((height, PW), F32)
    after2 = after1
    warped[pieces] = jnp.concatenate([after1, metadata(-1, 0)], axis=0).astype(BF16)
    for p in reversed(range(pieces)):
        block = slice(p * PW, (p + 1) * PW)
        tall = extended[:, block]
        upper = pltpu.roll(tall, lax.rem(rise, height + HALO), 0)[0:height]
        lower = pltpu.roll(tall, rise - 1, 0)[0:height]
        rows = ((1.0 - weight) * upper + weight * lower).astype(BF16).astype(F32)
        rolled1 = pltpu.roll(rows, turn1, 1)
        rolled2 = pltpu.roll(rows, turn2, 1)
        leftward = jnp.where(lane < PW - slide, rolled1, after1)
        rightward = jnp.where(lane < PW - 1 - slide, rolled2, after2)
        after1, after2 = rolled1, rolled2
        fraction = column_fraction[:, block].astype(F32)
        value = (1.0 - fraction) * leftward + fraction * rightward
        value = jnp.where(lane < piece_width[0, p], value, 0.0)
        warped[p] = jnp.concatenate(
            [value, metadata(route_cell[0, p], piece_width[0, p])], axis=0
        ).astype(BF16)

    def pack(index, carry):
        for k in range(PAIR):
            outgoing[index, k] = warped[chosen[index, k]]
        return carry

    lax.fori_loop(0, n, pack, 0)

    def piece_copy(index):
        return pltpu.make_async_remote_copy(
            src_ref=outgoing.at[index],
            dst_ref=incoming.at[index],
            send_sem=piece_send.at[index],
            recv_sem=piece_recv.at[index],
            device_id={"ccd": along(index)},
            device_id_type=MESH,
        )

    def send_piece(index, carry):
        piece_copy(index).start()
        return carry

    lax.fori_loop(1, n, send_piece, 0)
    incoming[0] = outgoing[0]

    for load in loads[8:]:
        load.wait()
    for r in range(height):
        tiles[r] = template[pl.ds(r // 8 * cells * 8 + r % 8, cells, stride=8), :].astype(BF16)
    template_copy = pltpu.make_async_remote_copy(
        src_ref=tiles.at[pl.ds(partner * (height - margin), margin)],
        dst_ref=source.at[pl.ds(band * (height + margin), margin)],
        send_sem=halo_send.at[1],
        recv_sem=halo_recv.at[1],
        device_id={"row": partner},
        device_id_type=MESH,
    )
    template_copy.start()
    source[margin : margin + height] = tiles[...]
    build_weights(match_kernel, taps, match_weight)
    build_windows(source, window, margin // QUAD, quads)
    build_windows(source, window, band * ((height + margin) // QUAD), margin // QUAD)
    template_copy.wait()
    build_windows(source, window, partner * ((height + margin) // QUAD), margin // QUAD)
    run_filter(window, match_weight, total, match_kernel.shape[0], quads, 0)
    build_weights(detection_kernel, taps, detect_weight)

    def take_piece(index, carry):
        piece_copy(index).wait_recv()
        return carry

    lax.fori_loop(1, n, take_piece, 0)
    chunk = cells // PAIR
    per_vreg = PW // SLOT
    lane_row = lax.broadcasted_iota(jnp.int32, (1, PW), 1)
    cell_of = lax.broadcasted_iota(jnp.int32, (cells, PAIR * chunk * SLOT), 0).astype(F32)
    k_row = lax.broadcasted_iota(jnp.int32, (1, PAIR * chunk * SLOT), 1) % SLOT
    placed_rows = list(range(height)) + [height + 1]
    live_total = jnp.zeros((1, PW), F32)
    placed = None
    for start in range(0, n, chunk):
        meta = [
            incoming[start + s // PAIR, s % PAIR, height : SLOT, :].astype(F32)
            for s in range(PAIR * chunk)
        ]
        for s in range(0, PAIR * chunk, PAIR):
            live_total = live_total + meta[s][2:3] * float(PW) + meta[s][3:4]
        parts = []
        for v in range(PAIR * chunk // per_vreg):
            part = meta[v * per_vreg + per_vreg - 1][0:1]
            for k in reversed(range(per_vreg - 1)):
                part = jnp.where(lane_row < (k + 1) * SLOT, meta[v * per_vreg + k][0:1], part)
            parts.append(part)
        cell_row = jnp.concatenate(parts, axis=1)
        placer = jnp.concatenate(
            [
                jnp.where(jnp.where(k_row == r, cell_row, -1.0) == cell_of, 1.0, 0.0).astype(BF16)
                for r in placed_rows
            ],
            axis=0,
        )
        block = incoming[start : start + chunk].reshape(PAIR * chunk * SLOT, PW)
        got = jnp.dot(placer, block, preferred_element_type=F32)
        placed = got if placed is None else placed + got
    width_of = placed[height * cells : (height + 1) * cells]
    live = lax.broadcasted_iota(jnp.int32, (cells, PW), 1).astype(F32) < width_of
    squares = jnp.zeros((cells, PW), F32)
    for r in range(height):
        d = placed[r * cells : (r + 1) * cells] - filtered_row(total, r, cells)
        d = jnp.where(live, d, 0.0)
        difference[pl.ds(r // 8 * cells * 8 + r % 8, cells, stride=8), :] = d
        squares = squares + d * d
        rounded[lead + r] = d.astype(BF16)
    partials[0] = jnp.sum(squares.reshape(cells // 8, 8, PW), axis=0)

    def noise_copy(index):
        return pltpu.make_async_remote_copy(
            src_ref=partials.at[0],
            dst_ref=partials.at[index],
            send_sem=noise_send.at[index],
            recv_sem=noise_recv.at[index],
            device_id=peer(index),
            device_id_type=MESH,
        )

    def send_noise(index, carry):
        noise_copy(index).start()
        return carry

    lax.fori_loop(1, everyone, send_noise, 0)

    difference_copy = pltpu.make_async_remote_copy(
        src_ref=rounded.at[pl.ds(lead + partner * (height - margin2), margin2)],
        dst_ref=rounded.at[pl.ds(lead - margin2 + band * (height + margin2), margin2)],
        send_sem=halo_send.at[2],
        recv_sem=halo_recv.at[2],
        device_id={"row": partner},
        device_id_type=MESH,
    )
    difference_copy.start()

    build_windows(rounded, window2, lead // QUAD, quads)
    build_windows(rounded, window2, band * ((height + lead) // QUAD), lead // QUAD)
    difference_copy.wait()
    build_windows(rounded, window2, partner * ((height + lead) // QUAD), lead // QUAD)
    run_filter(window2, detect_weight, total, detection_kernel.shape[0], quads, lead - margin2)

    def take_noise(index, carry):
        noise_copy(index).wait()
        return carry

    lax.fori_loop(1, everyone, take_noise, 0)

    def end_piece(index, carry):
        piece_copy(index).wait_send()
        return carry

    lax.fori_loop(1, n, end_piece, 0)

    squares = jnp.sum(partials[...], axis=0)
    square_sum = jnp.sum(jnp.sum(squares, axis=0, keepdims=True), axis=1, keepdims=True)
    live_count = live_total[:, 0:1] * float(2 * height)
    noise = square_sum / live_count
    detect = detection_kernel[...].astype(F32)
    norm = jnp.sum(jnp.sum(detect * detect, axis=0, keepdims=True), axis=1, keepdims=True)
    scale = 1.0 / jnp.sqrt(1.0 + noise * norm)
    scale = jnp.broadcast_to(scale, (cells, PW))
    for r in range(height):
        significance[pl.ds(r // 8 * cells * 8 + r % 8, cells, stride=8), :] = (
            filtered_row(total, r, cells) * scale
        )
    noise_out[...] = noise


def on_device(
    n,
    exposure,
    row_shift,
    row_fraction,
    column_shift,
    column_fraction,
    piece_width,
    route_tile,
    route_cell,
    template,
    match_kernel,
    detection_kernel,
):
    height, columns = exposure.shape[1:]
    pieces = columns // PW
    cells = template.shape[2] // PW
    extent = match_kernel.shape[1]
    extent2 = detection_kernel.shape[1]
    rows = height + 2 * (extent // 2)
    rows2 = height + 2 * QUAD * -(-(extent2 // 2) // QUAD)
    anywhere = pl.BlockSpec(memory_space=pl.ANY)
    vmem = pl.BlockSpec(memory_space=pltpu.VMEM)
    tiles = template.reshape(height // 8, 8, cells, PW).transpose(0, 2, 1, 3).reshape(height * cells, PW)
    difference, significance, noise = pl.pallas_call(
        functools.partial(step_kernel, n),
        out_shape=(
            jax.ShapeDtypeStruct((height * cells, PW), F32),
            jax.ShapeDtypeStruct((height * cells, PW), F32),
            jax.ShapeDtypeStruct((1, 1), F32),
        ),
        in_specs=[anywhere] * 11,
        out_specs=(vmem, vmem, vmem),
        scratch_shapes=[
            pltpu.SMEM(row_shift.shape, jnp.int32),
            pltpu.SMEM(column_shift.shape, jnp.int32),
            pltpu.SMEM(piece_width.shape, jnp.int32),
            pltpu.SMEM(route_tile.shape, jnp.int32),
            pltpu.SMEM(route_cell.shape, jnp.int32),
            pltpu.VMEM(row_fraction.shape, BF16),
            pltpu.VMEM(column_fraction.shape, BF16),
            pltpu.VMEM((height * cells, PW), F32),
            pltpu.VMEM((extent, extent), BF16),
            pltpu.VMEM((extent2, extent2), BF16),
            pltpu.SMEM((n, PAIR), jnp.int32),
            pltpu.VMEM((height + HALO, columns), F32),
            pltpu.VMEM((pieces + 1, SLOT, PW), BF16),
            pltpu.VMEM((n, PAIR, SLOT, PW), BF16),
            pltpu.VMEM((n, PAIR, SLOT, PW), BF16),
            pltpu.VMEM((height, cells, PW), BF16),
            pltpu.VMEM((rows, cells, PW), BF16),
            pltpu.VMEM((rows // QUAD, QUAD, 2 * cells, PW), BF16),
            pltpu.VMEM(((extent + QUAD - 1) * PW, 2 * PW), BF16),
            pltpu.VMEM(((extent2 + QUAD - 1) * PW, 2 * PW), BF16),
            pltpu.VMEM((extent + 15, PW), F32),
            pltpu.VMEM((height // QUAD * 2 * cells, 2 * PW), F32),
            pltpu.VMEM((rows2, cells, PW), BF16),
            pltpu.VMEM((rows2 // QUAD, QUAD, 2 * cells, PW), BF16),
            pltpu.VMEM((2 * n, 8, PW), F32),
            pltpu.SemaphoreType.DMA((11,)),
            pltpu.SemaphoreType.DMA((3,)),
            pltpu.SemaphoreType.DMA((3,)),
            pltpu.SemaphoreType.DMA((n,)),
            pltpu.SemaphoreType.DMA((n,)),
            pltpu.SemaphoreType.DMA((2 * n,)),
            pltpu.SemaphoreType.DMA((2 * n,)),
        ],
        compiler_params=pltpu.CompilerParams(
            collective_id=0, has_side_effects=True, vmem_limit_bytes=62 * 2**20
        ),
    )(
        row_shift,
        column_shift,
        piece_width,
        route_tile,
        route_cell,
        exposure[0],
        row_fraction,
        column_fraction,
        tiles,
        match_kernel[0],
        detection_kernel[0],
    )

    def as_rows(x):
        x = x.reshape(height // 8, cells, 8, PW).transpose(0, 2, 1, 3)
        return x.reshape(1, height, cells * PW)

    return (as_rows(difference), as_rows(significance), noise.reshape(()))


def solution(mesh):
    assert mesh.shape["row"] == 2
    return jax.shard_map(
        functools.partial(on_device, mesh.shape["ccd"]),
        mesh=mesh,
        in_specs=(
            P("ccd", "row", None),
            P("ccd"),
            P("ccd", "row"),
            P("ccd"),
            P("ccd", None),
            P("ccd", None),
            P("ccd", None),
            P("ccd", None),
            P("ccd", "row", None),
            P("ccd", None, None),
            P("ccd", None, None),
        ),
        out_specs=(P("ccd", "row", None), P("ccd", "row", None), P()),
        check_vma=False,
    )
```

```python
import functools

import jax
import jax.numpy as jnp
from jax import lax
from jax.experimental import pallas as pl
from jax.experimental.pallas import tpu as pltpu
from jax.sharding import PartitionSpec as P

PW = 128
PAIR = 2
HALO = 8
SLOT = 32
QUAD = 4
HALF = PW // 2
GROUP = 6
F32 = jnp.float32
BF16 = jnp.bfloat16
MESH = pl.DeviceIdType.MESH


def taps_by_lane(kernel, margin):
    extent = kernel.shape[0]
    b = lax.broadcasted_iota(jnp.int32, (extent, PW), 0)
    lane = lax.broadcasted_iota(jnp.int32, (extent, PW), 1)
    want = margin - b
    want = jnp.where(want < 0, want + PW, want)
    return jnp.dot(kernel, (lane == want).astype(BF16), preferred_element_type=F32)


def build_weights(kernel_ref, taps_ref, weight_ref):
    extent = kernel_ref.shape[0]
    margin = extent // 2
    taps_ref[...] = jnp.zeros_like(taps_ref)
    taps_ref[8 : 8 + extent, :] = taps_by_lane(kernel_ref[...], margin)
    lane = lax.broadcasted_iota(jnp.int32, (PW, PW), 1)
    nothing = jnp.zeros((2 * PW, PW), BF16)
    weight_ref[0 : 2 * PW, PW : 2 * PW] = nothing
    weight_ref[(extent + 1) * PW : (extent + 3) * PW, 0:PW] = nothing

    def circulant(u):
        row = jnp.broadcast_to(taps_ref[pl.ds(u + 8, 1), :], (PW, PW))
        return pltpu.roll(row, 0, 1, stride=1, stride_axis=0)

    def place(u, first, second):
        second = jnp.concatenate([second[HALF:], second[:HALF]], axis=0)
        both = jnp.where(lane < HALF, first, second).astype(BF16)
        at = pl.multiple_of(u * PW, PW)
        weight_ref[pl.ds(at, PW), 0:PW] = both
        at = pl.multiple_of((u + 2) * PW, PW)
        weight_ref[pl.ds(at, PW), PW : 2 * PW] = both

    def step(index, before):
        u = 2 * index
        now = circulant(u)
        after = circulant(u + 1)
        place(u, now, before)
        place(u + 1, after, now)
        return after

    lax.fori_loop(0, (extent + 1) // 2, step, jnp.zeros((PW, PW), F32))


def build_windows(source_ref, window_ref, first, count):
    rows, cells, _ = source_ref.shape

    def step(index, carry):
        q = first + index
        x = source_ref[pl.ds(q * QUAD, QUAD)].astype(F32).reshape(QUAD * cells, PW)
        lane = lax.broadcasted_iota(jnp.int32, x.shape, 1)
        cell = lax.broadcasted_iota(jnp.int32, x.shape, 0) % cells
        before = jnp.where(cell == 0, 0.0, pltpu.roll(x, 1, 0))
        after = jnp.where(cell == cells - 1, 0.0, pltpu.roll(x, x.shape[0] - 1, 0))
        even = jnp.where(lane < PW - HALF // 2, x, before)
        odd = pltpu.roll(jnp.where(lane >= HALF // 2, x, after), HALF, 1)
        window_ref[q, :, 0:cells, :] = even.astype(BF16).reshape(QUAD, cells, PW)
        window_ref[q, :, cells : 2 * cells, :] = odd.astype(BF16).reshape(QUAD, cells, PW)
        return carry

    lax.fori_loop(0, count, step, 0)


def run_filter(window_ref, weight_ref, sum_ref, extent, quads, skip):
    reach = extent + QUAD - 1
    blocks = window_ref.shape[2]
    for start in range(0, reach, GROUP):
        stop = min(start + GROUP, reach)
        left = jnp.concatenate(
            [
                window_ref[(u + skip) // QUAD : (u + skip) // QUAD + quads, (u + skip) % QUAD].reshape(quads * blocks, PW)
                for u in range(start, stop)
            ],
            axis=1,
        )
        part = jnp.dot(left, weight_ref[start * PW : stop * PW, :], preferred_element_type=F32)
        if start == 0:
            sum_ref[...] = part
        else:
            sum_ref[...] += part


def filtered_row(sum_ref, row, cells):
    quad, r = divmod(row, QUAD)
    at = quad * 2 * cells
    columns = slice((r // 2) * PW, (r // 2 + 1) * PW)
    even = sum_ref[at : at + cells, columns]
    odd = sum_ref[at + cells : at + 2 * cells, columns]
    lane = lax.broadcasted_iota(jnp.int32, (cells, PW), 1)
    if r % 2 == 0:
        return jnp.where(lane < HALF, even, pltpu.roll(odd, HALF, 1))
    return jnp.where(lane < HALF, pltpu.roll(even, HALF, 1), odd)


def step_kernel(
    n,
    row_shift_hbm,
    column_shift_hbm,
    piece_width_hbm,
    route_tile_hbm,
    route_cell_hbm,
    exposure_hbm,
    row_fraction_hbm,
    column_fraction_hbm,
    template_hbm,
    match_kernel_hbm,
    detection_kernel_hbm,
    difference,
    significance,
    noise_out,
    row_shift,
    column_shift,
    piece_width,
    route_tile,
    route_cell,
    row_fraction,
    column_fraction,
    template,
    match_kernel,
    detection_kernel,
    chosen,
    extended,
    warped,
    outgoing,
    incoming,
    tiles,
    source,
    window,
    match_weight,
    detect_weight,
    taps,
    total,
    rounded,
    window2,
    partials,
    load_sem,
    halo_send,
    halo_recv,
    piece_send,
    piece_recv,
    noise_send,
    noise_recv,
):
    height, columns = exposure_hbm.shape
    loads = [
        pltpu.make_async_copy(a, b, load_sem.at[k])
        for k, (a, b) in enumerate(
            [
                (exposure_hbm, extended.at[0:height]),
                (route_tile_hbm, route_tile),
                (route_cell_hbm, route_cell),
                (piece_width_hbm, piece_width),
                (row_shift_hbm, row_shift),
                (column_shift_hbm, column_shift),
                (row_fraction_hbm, row_fraction),
                (column_fraction_hbm, column_fraction),
                (template_hbm, template),
                (match_kernel_hbm, match_kernel),
                (detection_kernel_hbm, detection_kernel),
            ]
        )
    ]
    for load in loads:
        load.start()
    me = lax.axis_index("ccd")
    band = lax.axis_index("row")
    partner = 1 - band
    pieces = columns // PW
    cells = template.shape[0] // height
    margin = match_kernel.shape[0] // 2
    margin2 = detection_kernel.shape[0] // 2
    quads = height // QUAD
    everyone = 2 * n
    rows2 = rounded.shape[0]
    lead = rows2 // 2 - height // 2

    def peer(index):
        other = index >= n
        at = me + jnp.where(other, index - n, index)
        return {
            "ccd": jnp.where(at >= n, at - n, at),
            "row": jnp.where(other, partner, band),
        }

    def along(index):
        at = me + index
        return jnp.where(at >= n, at - n, at)

    barrier = pltpu.get_barrier_semaphore()

    def greet(index, carry):
        pl.semaphore_signal(barrier, inc=1, device_id=peer(index), device_id_type=MESH)
        return carry

    lax.fori_loop(1, everyone, greet, 0)

    outer = jnp.zeros((margin, cells, PW), BF16)
    source[pl.ds(band * (height + margin), margin)] = outer
    for q in (0, 1, rows2 // QUAD - 2, rows2 // QUAD - 1):
        rounded[q * QUAD : (q + 1) * QUAD] = jnp.zeros((QUAD, cells, PW), BF16)
    loads[0].wait()
    pl.semaphore_wait(barrier, everyone - 1)

    exposure_copy = pltpu.make_async_remote_copy(
        src_ref=extended.at[0:HALO],
        dst_ref=extended.at[height : height + HALO],
        send_sem=halo_send.at[0],
        recv_sem=halo_recv.at[0],
        device_id={"row": partner},
        device_id_type=MESH,
    )
    exposure_copy.start()
    for load in loads[1:8]:
        load.wait()

    def choose(index, carry):
        tile = along(index)
        first = pieces
        second = pieces
        for p in reversed(range(pieces)):
            here = route_tile[0, p] == tile
            second = jnp.where(here, first, second)
            first = jnp.where(here, p, first)
        chosen[index, 0] = first
        chosen[index, 1] = second
        return carry

    lax.fori_loop(0, n, choose, 0)

    exposure_copy.wait()
    below = extended[height : height + HALO, :]
    extended[height : height + HALO, :] = jnp.where(band == 0, below, jnp.zeros_like(below))
    diagonal = lax.broadcasted_iota(jnp.int32, (height, height), 0) == lax.broadcasted_iota(
        jnp.int32, (height, height), 1
    )
    weight = jnp.sum(
        jnp.where(diagonal, jnp.broadcast_to(row_fraction[...].astype(F32), (height, height)), 0.0),
        axis=1,
        keepdims=True,
    )
    shift = row_shift[0]
    slide = column_shift[0]
    lane = lax.broadcasted_iota(jnp.int32, (height, PW), 1)
    all_widths = piece_width[0, 0]
    for p in range(1, pieces):
        all_widths = all_widths + piece_width[0, p]
    meta_row = lax.broadcasted_iota(jnp.int32, (SLOT - height, PW), 0)

    def metadata(cell, width):
        m = jnp.where(meta_row == 0, cell, 0)
        m = jnp.where(meta_row == 1, width, m)
        m = jnp.where(meta_row == 2, all_widths // PW, m)
        m = jnp.where(meta_row == 3, all_widths % PW, m)
        return m.astype(F32)

    rise = height + HALO - shift
    turn1 = lax.rem(PW - slide, PW)
    turn2 = PW - 1 - slide
    after1 = jnp.zeros((height, PW), F32)
    after2 = after1
    warped[pieces] = jnp.concatenate([after1, metadata(-1, 0)], axis=0).astype(BF16)
    for p in reversed(range(pieces)):
        block = slice(p * PW, (p + 1) * PW)
        tall = extended[:, block]
        upper = pltpu.roll(tall, lax.rem(rise, height + HALO), 0)[0:height]
        lower = pltpu.roll(tall, rise - 1, 0)[0:height]
        rows = ((1.0 - weight) * upper + weight * lower).astype(BF16).astype(F32)
        rolled1 = pltpu.roll(rows, turn1, 1)
        rolled2 = pltpu.roll(rows, turn2, 1)
        leftward = jnp.where(lane < PW - slide, rolled1, after1)
        rightward = jnp.where(lane < PW - 1 - slide, rolled2, after2)
        after1, after2 = rolled1, rolled2
        fraction = column_fraction[:, block].astype(F32)
        value = (1.0 - fraction) * leftward + fraction * rightward
        value = jnp.where(lane < piece_width[0, p], value, 0.0)
        warped[p] = jnp.concatenate(
            [value, metadata(route_cell[0, p], piece_width[0, p])], axis=0
        ).astype(BF16)

    def pack(index, carry):
        for k in range(PAIR):
            outgoing[index, k] = warped[chosen[index, k]]
        return carry

    lax.fori_loop(0, n, pack, 0)

    def piece_copy(index):
        return pltpu.make_async_remote_copy(
            src_ref=outgoing.at[index],
            dst_ref=incoming.at[index],
            send_sem=piece_send.at[index],
            recv_sem=piece_recv.at[index],
            device_id={"ccd": along(index)},
            device_id_type=MESH,
        )

    def send_piece(index, carry):
        piece_copy(index).start()
        return carry

    lax.fori_loop(1, n, send_piece, 0)
    incoming[0] = outgoing[0]

    for load in loads[8:]:
        load.wait()
    for r in range(height):
        tiles[r] = template[pl.ds(r // 8 * cells * 8 + r % 8, cells, stride=8), :].astype(BF16)
    template_copy = pltpu.make_async_remote_copy(
        src_ref=tiles.at[pl.ds(partner * (height - margin), margin)],
        dst_ref=source.at[pl.ds(band * (height + margin), margin)],
        send_sem=halo_send.at[1],
        recv_sem=halo_recv.at[1],
        device_id={"row": partner},
        device_id_type=MESH,
    )
    template_copy.start()
    source[margin : margin + height] = tiles[...]
    build_weights(match_kernel, taps, match_weight)
    build_windows(source, window, margin // QUAD, quads)
    build_windows(source, window, band * ((height + margin) // QUAD), margin // QUAD)
    template_copy.wait()
    build_windows(source, window, partner * ((height + margin) // QUAD), margin // QUAD)
    run_filter(window, match_weight, total, match_kernel.shape[0], quads, 0)
    build_weights(detection_kernel, taps, detect_weight)

    def take_piece(index, carry):
        piece_copy(index).wait_recv()
        return carry

    lax.fori_loop(1, n, take_piece, 0)
    chunk = cells // PAIR
    per_vreg = PW // SLOT
    lane_row = lax.broadcasted_iota(jnp.int32, (1, PW), 1)
    cell_of = lax.broadcasted_iota(jnp.int32, (cells, PAIR * chunk * SLOT), 0).astype(F32)
    k_row = lax.broadcasted_iota(jnp.int32, (1, PAIR * chunk * SLOT), 1) % SLOT
    placed_rows = list(range(height)) + [height + 1]
    live_total = jnp.zeros((1, PW), F32)
    placed = None
    for start in range(0, n, chunk):
        meta = [
            incoming[start + s // PAIR, s % PAIR, height : SLOT, :].astype(F32)
            for s in range(PAIR * chunk)
        ]
        for s in range(0, PAIR * chunk, PAIR):
            live_total = live_total + meta[s][2:3] * float(PW) + meta[s][3:4]
        parts = []
        for v in range(PAIR * chunk // per_vreg):
            part = meta[v * per_vreg + per_vreg - 1][0:1]
            for k in reversed(range(per_vreg - 1)):
                part = jnp.where(lane_row < (k + 1) * SLOT, meta[v * per_vreg + k][0:1], part)
            parts.append(part)
        cell_row = jnp.concatenate(parts, axis=1)
        placer = jnp.concatenate(
            [
                jnp.where(jnp.where(k_row == r, cell_row, -1.0) == cell_of, 1.0, 0.0).astype(BF16)
                for r in placed_rows
            ],
            axis=0,
        )
        block = incoming[start : start + chunk].reshape(PAIR * chunk * SLOT, PW)
        got = jnp.dot(placer, block, preferred_element_type=F32)
        placed = got if placed is None else placed + got
    width_of = placed[height * cells : (height + 1) * cells]
    live = lax.broadcasted_iota(jnp.int32, (cells, PW), 1).astype(F32) < width_of
    squares = jnp.zeros((cells, PW), F32)
    for r in range(height):
        d = placed[r * cells : (r + 1) * cells] - filtered_row(total, r, cells)
        d = jnp.where(live, d, 0.0)
        difference[pl.ds(r // 8 * cells * 8 + r % 8, cells, stride=8), :] = d
        squares = squares + d * d
        rounded[lead + r] = d.astype(BF16)
    partials[0, 0:1] = jnp.sum(squares, axis=0, keepdims=True)

    def noise_copy(index):
        return pltpu.make_async_remote_copy(
            src_ref=partials.at[0, 0:1],
            dst_ref=partials.at[index, 0:1],
            send_sem=noise_send.at[index],
            recv_sem=noise_recv.at[index],
            device_id=peer(index),
            device_id_type=MESH,
        )

    def send_noise(index, carry):
        noise_copy(index).start()
        return carry

    lax.fori_loop(1, everyone, send_noise, 0)

    difference_copy = pltpu.make_async_remote_copy(
        src_ref=rounded.at[pl.ds(lead + partner * (height - margin2), margin2)],
        dst_ref=rounded.at[pl.ds(lead - margin2 + band * (height + margin2), margin2)],
        send_sem=halo_send.at[2],
        recv_sem=halo_recv.at[2],
        device_id={"row": partner},
        device_id_type=MESH,
    )
    difference_copy.start()

    build_windows(rounded, window2, lead // QUAD, quads)
    build_windows(rounded, window2, band * ((height + lead) // QUAD), lead // QUAD)
    difference_copy.wait()
    build_windows(rounded, window2, partner * ((height + lead) // QUAD), lead // QUAD)
    run_filter(window2, detect_weight, total, detection_kernel.shape[0], quads, lead - margin2)

    def take_noise(index, carry):
        noise_copy(index).wait()
        return carry

    lax.fori_loop(1, everyone, take_noise, 0)

    def end_piece(index, carry):
        piece_copy(index).wait_send()
        return carry

    lax.fori_loop(1, n, end_piece, 0)

    squares = jnp.sum(partials[:, 0:1, :], axis=0)
    square_sum = jnp.sum(jnp.sum(squares, axis=0, keepdims=True), axis=1, keepdims=True)
    live_count = live_total[:, 0:1] * float(2 * height)
    noise = square_sum / live_count
    detect = detection_kernel[...].astype(F32)
    norm = jnp.sum(jnp.sum(detect * detect, axis=0, keepdims=True), axis=1, keepdims=True)
    scale = 1.0 / jnp.sqrt(1.0 + noise * norm)
    scale = jnp.broadcast_to(scale, (cells, PW))
    for r in range(height):
        significance[pl.ds(r // 8 * cells * 8 + r % 8, cells, stride=8), :] = (
            filtered_row(total, r, cells) * scale
        )
    noise_out[...] = noise


def on_device(
    n,
    exposure,
    row_shift,
    row_fraction,
    column_shift,
    column_fraction,
    piece_width,
    route_tile,
    route_cell,
    template,
    match_kernel,
    detection_kernel,
):
    height, columns = exposure.shape[1:]
    pieces = columns // PW
    cells = template.shape[2] // PW
    extent = match_kernel.shape[1]
    extent2 = detection_kernel.shape[1]
    rows = height + 2 * (extent // 2)
    rows2 = height + 2 * QUAD * -(-(extent2 // 2) // QUAD)
    anywhere = pl.BlockSpec(memory_space=pl.ANY)
    vmem = pl.BlockSpec(memory_space=pltpu.VMEM)
    tiles = template.reshape(height // 8, 8, cells, PW).transpose(0, 2, 1, 3).reshape(height * cells, PW)
    difference, significance, noise = pl.pallas_call(
        functools.partial(step_kernel, n),
        out_shape=(
            jax.ShapeDtypeStruct((height * cells, PW), F32),
            jax.ShapeDtypeStruct((height * cells, PW), F32),
            jax.ShapeDtypeStruct((1, 1), F32),
        ),
        in_specs=[anywhere] * 11,
        out_specs=(vmem, vmem, vmem),
        scratch_shapes=[
            pltpu.SMEM(row_shift.shape, jnp.int32),
            pltpu.SMEM(column_shift.shape, jnp.int32),
            pltpu.SMEM(piece_width.shape, jnp.int32),
            pltpu.SMEM(route_tile.shape, jnp.int32),
            pltpu.SMEM(route_cell.shape, jnp.int32),
            pltpu.VMEM(row_fraction.shape, BF16),
            pltpu.VMEM(column_fraction.shape, BF16),
            pltpu.VMEM((height * cells, PW), F32),
            pltpu.VMEM((extent, extent), BF16),
            pltpu.VMEM((extent2, extent2), BF16),
            pltpu.SMEM((n, PAIR), jnp.int32),
            pltpu.VMEM((height + HALO, columns), F32),
            pltpu.VMEM((pieces + 1, SLOT, PW), BF16),
            pltpu.VMEM((n, PAIR, SLOT, PW), BF16),
            pltpu.VMEM((n, PAIR, SLOT, PW), BF16),
            pltpu.VMEM((height, cells, PW), BF16),
            pltpu.VMEM((rows, cells, PW), BF16),
            pltpu.VMEM((rows // QUAD, QUAD, 2 * cells, PW), BF16),
            pltpu.VMEM(((extent + QUAD - 1) * PW, 2 * PW), BF16),
            pltpu.VMEM(((extent2 + QUAD - 1) * PW, 2 * PW), BF16),
            pltpu.VMEM((extent + 15, PW), F32),
            pltpu.VMEM((height // QUAD * 2 * cells, 2 * PW), F32),
            pltpu.VMEM((rows2, cells, PW), BF16),
            pltpu.VMEM((rows2 // QUAD, QUAD, 2 * cells, PW), BF16),
            pltpu.VMEM((2 * n, 8, PW), F32),
            pltpu.SemaphoreType.DMA((11,)),
            pltpu.SemaphoreType.DMA((3,)),
            pltpu.SemaphoreType.DMA((3,)),
            pltpu.SemaphoreType.DMA((n,)),
            pltpu.SemaphoreType.DMA((n,)),
            pltpu.SemaphoreType.DMA((2 * n,)),
            pltpu.SemaphoreType.DMA((2 * n,)),
        ],
        compiler_params=pltpu.CompilerParams(
            collective_id=0, has_side_effects=True, vmem_limit_bytes=62 * 2**20
        ),
    )(
        row_shift,
        column_shift,
        piece_width,
        route_tile,
        route_cell,
        exposure[0],
        row_fraction,
        column_fraction,
        tiles,
        match_kernel[0],
        detection_kernel[0],
    )

    def as_rows(x):
        x = x.reshape(height // 8, cells, 8, PW).transpose(0, 2, 1, 3)
        return x.reshape(1, height, cells * PW)

    return (as_rows(difference), as_rows(significance), noise.reshape(()))


def solution(mesh):
    assert mesh.shape["row"] == 2
    return jax.shard_map(
        functools.partial(on_device, mesh.shape["ccd"]),
        mesh=mesh,
        in_specs=(
            P("ccd", "row", None),
            P("ccd"),
            P("ccd", "row"),
            P("ccd"),
            P("ccd", None),
            P("ccd", None),
            P("ccd", None),
            P("ccd", None),
            P("ccd", "row", None),
            P("ccd", None, None),
            P("ccd", None, None),
        ),
        out_specs=(P("ccd", "row", None), P("ccd", "row", None), P()),
        check_vma=False,
    )
```
